32 devices in a mesh: cache: 8 (over z, y), group: 4 (over x, core).
Axes of the slice: x: 2, y: 2, z: 4, core: 2. Of those that a mesh axis runs over, the one named last changes fastest.
Arguments:
- queries: bfloat16 [32, 4096], P('cache'), may hold values from -240 to 240
- request_of: int32 [32], P('cache'), may hold values from 0 to 1, as said below
- selected: int32 [32, 8, 4], P('cache', 'group'), may hold values from 0 to 15, as said below
- cache_keys: bfloat16 [2, 8, 2048, 128], P(None, 'group', 'cache'), may hold values from -6 to 6
- cache_values: bfloat16 [2, 8, 2048, 128], P(None, 'group', 'cache'), may hold values from -6 to 6
- recent_keys: bfloat16 [32, 8, 1024, 128], P('cache', None, 'group'), may hold values from -6 to 6
- recent_values: bfloat16 [32, 8, 1024, 128], P('cache', None, 'group'), may hold values from -6 to 6
Outputs:
- attended: bfloat16 [32, 4096], P('cache', 'group')
The draws below stay inside these ranges and needn't reach their ends.
Inputs may be any that keep to these rules, and one draw needn't show every extreme that they name: `request_of`: each prompt is read by exactly 16 slots. `selected`: for each slot and key-value head the 4 block ids have distinct owners id // 2; the 4 slots of one index of cache, with the key-value heads of one index of group, select at most 4 blocks held by any one owner, and exactly 4 from some owner.
All inputs are finite; a program needn't handle non-finite values.
Results may differ from the reference program's by a relative error of at most 0.0015.
Values may be sent and summed in bfloat16 or wider, within the bound.
No kernel may reach another device: no remote copies, remote signals or barrier semaphores. Data moves between devices by JAX's collectives and lax.ppermute only.
A program may use at most 64 MiB of HBM per device.

```python
import jax
import jax.numpy as jnp
from jax import lax

QH = 32
KVH = 8
HD = 128
BLOCK = 128
TOPK = 4
RECENT = 1024
REQ_GRP = 4
BLK_DEV = 2
REQS = 32
PROMPTS = 2
NBLK = 16
N_CACHE = 8
N_GROUP = 4


def draw_queries(key, part):
    base_key = jax.random.fold_in(jax.random.fold_in(key, 7), 0)
    base = jnp.clip(jax.random.normal(base_key, (REQS, QH, HD), jnp.float32), -6.0, 6.0)
    return base.reshape(REQS, QH * HD).astype(jnp.bfloat16)


def draw_request_of(key, part):
    order = jax.random.permutation(jax.random.fold_in(key, 13), REQS)
    return (order.astype(jnp.int32) % PROMPTS).astype(jnp.int32)


def draw_selected(key, part):
    mine_heads = KVH // N_GROUP
    wanted = REQ_GRP * mine_heads * TOPK
    order_key, local_key = jax.random.split(jax.random.fold_in(key, 11))
    scores = jax.random.randint(order_key, (N_CACHE, N_GROUP, N_CACHE), 0, 65536).astype(jnp.int32)
    scores = scores * N_CACHE + jnp.arange(N_CACHE, dtype=jnp.int32)
    owner_order = jnp.argsort(scores, axis=-1, stable=True).astype(jnp.int32)
    position = jnp.arange(wanted, dtype=jnp.int32) % N_CACHE
    owners = owner_order[:, :, position]
    owners = owners.reshape(N_CACHE, N_GROUP, REQ_GRP, mine_heads, TOPK)
    owners = jnp.transpose(owners, (0, 2, 1, 3, 4)).reshape(REQS, KVH, TOPK)
    local_block = jax.random.randint(local_key, (REQS, KVH, TOPK), 0, BLK_DEV).astype(jnp.int32)
    return (owners * BLK_DEV + local_block).astype(jnp.int32)


def block_levels(own_key, dims, shards, least, largest):
    level, own = 1.0, jax.random.fold_in(own_key, 6)
    for axis_at, parts in shards:
        heights = jnp.exp(jax.random.uniform(jax.random.fold_in(own, axis_at), (parts,), jnp.float32, least / len(shards), largest / len(shards)))
        level = level * jnp.repeat(heights, dims[axis_at] // parts).reshape([-1 if axis == axis_at else 1 for axis in range(len(dims))])
    return level


def normal_values(key, extent, scale, most, shards=(), kind=jnp.bfloat16):
    gain = block_levels(key, extent, shards, -0.22, 0.18) if shards else 1.0
    values = jax.random.normal(key, extent, jnp.float32) * scale * gain
    return jnp.minimum(jnp.maximum(values, -most), most).astype(kind)


def setup_inputs(seed: int = 0) -> dict:
    keys = jax.random.split(jax.random.key(seed), 8)
    return {
        "queries": draw_queries(jax.random.fold_in(keys[7], 71), 0),
        "request_of": draw_request_of(jax.random.fold_in(keys[7], 71), 0),
        "selected": draw_selected(jax.random.fold_in(keys[7], 71), 0),
        "cache_keys": normal_values(keys[3], (PROMPTS, KVH, NBLK * BLOCK, HD), 1.0, 6.0, ((1, 4), (2, 8))),
        "cache_values": normal_values(keys[4], (PROMPTS, KVH, NBLK * BLOCK, HD), 1.0, 6.0, ((1, 4), (2, 8))),
        "recent_keys": normal_values(keys[5], (REQS, KVH, RECENT, HD), 1.0, 6.0, ((0, 8), (2, 4))),
        "recent_values": normal_values(keys[6], (REQS, KVH, RECENT, HD), 1.0, 6.0, ((0, 8), (2, 4))),
    }


def reference(queries, request_of, selected, cache_keys, cache_values, recent_keys, recent_values):
    per_kv = QH // KVH
    score_scale = HD ** -0.5
    head_index = jnp.arange(KVH, dtype=jnp.int32)[:, None]

    def per_slot(slot):
        request = request_of[slot]
        selection = selected[slot]
        key_blocks = cache_keys[request].reshape(KVH, NBLK, BLOCK, HD)
        value_blocks = cache_values[request].reshape(KVH, NBLK, BLOCK, HD)
        picked_keys = key_blocks[head_index, selection].reshape(KVH, TOPK * BLOCK, HD)
        picked_values = value_blocks[head_index, selection].reshape(KVH, TOPK * BLOCK, HD)
        key_rows = jnp.concatenate([picked_keys, recent_keys[slot]], axis=1).astype(jnp.float32)
        value_rows = jnp.concatenate([picked_values, recent_values[slot]], axis=1).astype(jnp.float32)
        query_heads = queries[slot].reshape(KVH, per_kv, HD).astype(jnp.float32)
        scores = jnp.einsum("hgd,hnd->hgn", query_heads, key_rows, precision=lax.Precision.HIGHEST) * score_scale
        weights = jax.nn.softmax(scores, axis=-1)
        result = jnp.einsum("hgn,hnd->hgd", weights, value_rows, precision=lax.Precision.HIGHEST)
        return result.reshape(QH * HD).astype(jnp.bfloat16)

    return lax.map(per_slot, jnp.arange(REQS, dtype=jnp.int32))
```

```python
import jax
import jax.numpy as jnp
from jax import lax
from jax.sharding import PartitionSpec as P

BLOCK = 128
LOW = -1e30
DENSE_LIMIT = 1 << 20


def weighted(exponent, value_rows, spec):
    high = lax.reduce_precision(exponent, 8, 7)
    rest = (exponent - high).astype(jnp.bfloat16)
    both = jnp.stack([high.astype(jnp.bfloat16), rest])
    out = jnp.einsum(spec, both, value_rows, preferred_element_type=jnp.float32)
    return out[0] + out[1]


def pack(summed, highest, totals):
    lead = summed.shape[0]
    rows = summed.shape[1]
    lanes = summed.shape[2]
    extra = jnp.concatenate([highest, totals], axis=1)
    want = -(-2 * rows // lanes) * lanes
    extra = jnp.pad(extra, ((0, 0), (0, want - 2 * rows))).reshape(lead, want // lanes, lanes)
    return jnp.concatenate([summed, extra], axis=1)


def unpack(packed, rows):
    lead = packed.shape[0]
    extra = packed[:, rows:].reshape(lead, -1)
    return packed[:, :rows], extra[:, :rows], extra[:, rows : 2 * rows]


def per_device(queries, request_of, selected, cache_keys, cache_values, recent_keys, recent_values):
    row_count = queries.shape[0]
    heads_kv = recent_keys.shape[1]
    head_dim = recent_keys.shape[3]
    per_kv = queries.shape[1] // (heads_kv * head_dim)
    mine_heads = selected.shape[1]
    top_count = selected.shape[2]
    score_scale = head_dim ** (-0.5)
    owner_count = lax.axis_size("cache")
    group_count = lax.axis_size("group")
    prompt_count = cache_keys.shape[0]
    held = cache_keys.shape[2]
    per_owner = held // BLOCK
    rows = row_count * mine_heads * per_kv

    all_heads = queries.reshape(row_count, heads_kv, per_kv, head_dim)
    own_heads = lax.dynamic_slice_in_dim(
        all_heads, lax.axis_index("group") * mine_heads, mine_heads, 1
    )
    ids = jnp.concatenate(
        [selected, jnp.broadcast_to(request_of[:, None, None], (row_count, mine_heads, 1))], axis=2
    ).astype(jnp.bfloat16)
    ids = jnp.pad(ids, ((0, 0), (0, 0), (0, head_dim - top_count - 1)))
    ask = jnp.concatenate([own_heads, ids[:, :, None, :]], axis=2)
    ask = jnp.broadcast_to(ask[None], (owner_count,) + ask.shape)
    asked = lax.all_to_all(ask, "cache", split_axis=0, concat_axis=0, tiled=True)

    near_scores = (
        jnp.einsum("rhgd,rhnd->rhgn", all_heads, recent_keys, preferred_element_type=jnp.float32)
        * score_scale
    )
    near_highest = jnp.max(near_scores, axis=-1)
    near_exp = jnp.exp(near_scores - near_highest[..., None])
    near_totals = jnp.sum(near_exp, axis=-1)
    near_summed = weighted(near_exp, recent_values, "xrhgn,rhnd->xrhgd")

    def to_groups(array):
        array = array.reshape((row_count, group_count, mine_heads) + array.shape[2:])
        return jnp.moveaxis(array, 1, 0)

    near = pack(
        to_groups(near_summed).reshape(group_count, rows, head_dim),
        to_groups(near_highest).reshape(group_count, rows),
        to_groups(near_totals).reshape(group_count, rows),
    )
    near = lax.all_to_all(near, "group", split_axis=0, concat_axis=0, tiled=True)

    block = jnp.arange(per_owner, dtype=jnp.int32) + lax.axis_index("cache") * per_owner

    def far_attention(asked):
        far_heads = asked[:, :, :, :per_kv]
        far_ids = asked[:, :, :, per_kv, : top_count + 1].astype(jnp.int32)
        wants = jnp.any(far_ids[..., :top_count, None] == block, axis=3)
        prompt = far_ids[..., top_count, None] == jnp.arange(prompt_count, dtype=jnp.int32)
        wants = prompt[..., :, None] & wants[..., None, :]
        wants = jnp.broadcast_to(
            wants[:, :, :, None, :, :, None],
            wants.shape[:3] + (per_kv,) + wants.shape[3:] + (BLOCK,),
        ).reshape(wants.shape[:3] + (per_kv, prompt_count, held))
        scores = (
            jnp.einsum(
                "crhgd,phnd->crhgpn", far_heads, cache_keys, preferred_element_type=jnp.float32
            )
            * score_scale
        )
        scores = jnp.where(wants, scores, LOW)
        highest = jnp.max(scores, axis=(4, 5))
        exponent = jnp.where(wants, jnp.exp(scores - highest[..., None, None]), 0.0)
        totals = jnp.sum(exponent, axis=(4, 5))
        return weighted(exponent, cache_values, "xcrhgpn,phnd->xcrhgd"), highest, totals

    if owner_count * rows * prompt_count * held <= DENSE_LIMIT:
        far_summed, far_highest, far_totals = far_attention(asked)
    else:
        far_summed, far_highest, far_totals = lax.map(lambda one: far_attention(one[None]), asked)
    far = pack(
        far_summed.reshape(owner_count, rows, head_dim),
        far_highest.reshape(owner_count, rows),
        far_totals.reshape(owner_count, rows),
    )
    far = lax.all_to_all(far, "cache", split_axis=0, concat_axis=0, tiled=True)

    parts = jnp.concatenate([near, far], axis=0)
    summed, highest, totals = unpack(parts, rows)
    factor = jnp.exp(highest - jnp.max(highest, axis=0)[None])
    weight = jnp.sum(factor * totals, axis=0)
    merged = jnp.sum(factor[..., None] * summed, axis=0) / weight[..., None]
    return merged.reshape(row_count, mine_heads * per_kv * head_dim).astype(jnp.bfloat16)


def solution(mesh):
    return jax.shard_map(
        per_device,
        mesh=mesh,
        in_specs=(
            P("cache", None),
            P("cache"),
            P("cache", "group", None),
            P(None, "group", "cache", None),
            P(None, "group", "cache", None),
            P("cache", None, "group", None),
            P("cache", None, "group", None),
        ),
        out_specs=P("cache", "group"),
        check_vma=False,
    )
```

```python
import functools

import jax
import jax.numpy as jnp
from jax import lax
from jax.experimental import pallas as pl
from jax.experimental.pallas import tpu as pltpu
from jax.sharding import PartitionSpec as P

BLOCK = 128
LANES = 128
LOW = -1e30

ASK_FLOPS = 10**9
IN_VMEM = pl.BlockSpec(memory_space=pltpu.VMEM)
IN_HBM = pl.BlockSpec(memory_space=pl.ANY)


PARAMS = pltpu.CompilerParams(vmem_limit_bytes=16 * 1024 * 1024)


def stay(array):
    return pltpu.with_memory_space_constraint(array, pltpu.HBM)


def keep(array):
    return pltpu.with_memory_space_constraint(array, pltpu.VMEM)


def split_product(exponent, values_of, masks):
    rows = exponent.shape[0]
    high = exponent.astype(jnp.bfloat16).astype(jnp.float32)
    both = jnp.concatenate([high, exponent - high], axis=0)
    total = None
    for index, mask in enumerate(masks):
        part = jnp.where(jnp.concatenate([mask, mask], axis=0), both, 0.0).astype(jnp.bfloat16)
        term = jnp.dot(part, values_of(index), preferred_element_type=jnp.float32)
        total = term if total is None else total + term
    return total[:rows] + total[rows:]


def statistics(highest, totals, head, rows, lead):
    half_rows = rows // 2
    shape = (lead * rows, LANES)
    lane = lax.broadcasted_iota(jnp.int32, shape, 1)
    row = lax.broadcasted_iota(jnp.int32, shape, 0)
    place = 2 * head + (row % rows) // half_rows
    tile = jnp.where(lane == place, highest, 0.0) + jnp.where(
        lane == place + LANES // 2, totals, 0.0
    )
    tile = tile.reshape(lead, rows, LANES)
    return tile[:, :half_rows] + tile[:, half_rows:]


def ask_kernel(row_count, mine_heads, per_kv, top_count, per_owner, q_hbm, prompt_hbm, sel_hbm,
               out_ref, q_rows_ref, q_ref, prompt_ref, sel_ref, rows_ref, code_ref, sems):
    owner_count = out_ref.shape[0]
    rows = row_count * per_kv
    pairs = ((q_hbm, q_ref), (prompt_hbm, prompt_ref), (sel_hbm, sel_ref))
    copies = [
        pltpu.make_async_copy(source, target, sems.at[index])
        for index, (source, target) in enumerate(pairs)
    ]
    for copy in copies:
        copy.start()
    code_ref[...] = jnp.full(code_ref.shape, -1.0, jnp.float32)
    for copy in copies:
        copy.wait()
    for tile in range(q_ref.shape[1] // LANES):
        head, query = divmod(tile, per_kv)
        rows_ref[pl.ds(head * rows + query, row_count, stride=per_kv), :] = q_ref[
            :, tile * LANES : (tile + 1) * LANES
        ].astype(jnp.float32)
    q_rows_ref[...] = rows_ref[...].astype(q_rows_ref.dtype)
    for head in range(mine_heads):
        for row in range(row_count):
            at = (head * row_count + row) * per_kv
            for top in range(top_count):
                block = sel_ref[row, head, top]
                owner = block // per_owner
                code = prompt_ref[row] * per_owner + block % per_owner
                code_ref[owner, at : at + per_kv, :] = jnp.full(
                    (per_kv, LANES), code, jnp.int32
                ).astype(jnp.float32)
    first = pl.multiple_of(lax.axis_index("group") * (mine_heads * rows), mine_heads * rows)
    mine = rows_ref[pl.ds(first, mine_heads * rows), :].astype(out_ref.dtype)
    for owner in range(owner_count):
        out_ref[owner, :, :LANES] = mine
        out_ref[owner, :, LANES:] = code_ref[owner].astype(out_ref.dtype)


def near_kernel(row_count, mine_heads, per_kv, scale, q_ref, k_ref, v_hbm, *rest):
    outs, (v_ref, scores_ref, summed_ref, stats_ref, sems) = rest[:-5], rest[-5:]
    group_count = len(outs)
    heads = group_count * mine_heads
    me = lax.axis_index("group")
    rows = per_kv * row_count
    half = rows // 2
    copies = []
    for index in range(group_count):
        at = pl.ds(index * mine_heads, mine_heads)
        copies.append(pltpu.make_async_copy(v_hbm.at[:, at], v_ref.at[:, at], sems.at[index]))
        copies[index].start()
    slot = lax.broadcasted_iota(jnp.int32, (rows, 1), 0) // per_kv
    for head in range(heads):
        q = q_ref[head * rows : (head + 1) * rows, :]
        scores = None
        for row in range(row_count):
            part = lax.dot_general(
                q, k_ref[row, head], (((1,), (1,)), ((), ())), preferred_element_type=jnp.float32
            )
            scores = part if scores is None else jnp.where(slot == row, part, scores)
        scores_ref[head * rows : (head + 1) * rows, :] = scores
    scores = scores_ref[...] * scale
    highest = jnp.max(scores, axis=1, keepdims=True)
    exponent = jnp.exp(scores - highest)
    totals = jnp.sum(exponent, axis=1, keepdims=True)
    high = exponent.astype(jnp.bfloat16)
    rest_part = (exponent - high.astype(jnp.float32)).astype(jnp.bfloat16)
    for head in range(heads):
        if head % mine_heads == 0:
            copies[head // mine_heads].wait()
        at = slice(head * rows, (head + 1) * rows)
        both = jnp.concatenate([high[at], rest_part[at]], axis=0)
        summed = None
        for row in range(row_count):
            part = jnp.dot(both, v_ref[row, head], preferred_element_type=jnp.float32)
            part = part[:rows] + part[rows:]
            summed = part if summed is None else jnp.where(slot == row, part, summed)
        summed_ref[at, :] = summed
        tile = statistics(highest[at], totals[at], head % mine_heads, rows, 1)[0]
        at = slice(head // mine_heads * half, (head // mine_heads + 1) * half)
        stats_ref[at, :] = tile if head % mine_heads == 0 else stats_ref[at, :] + tile
    count = mine_heads * rows
    for step in range(group_count):
        peer = partner(me, step, group_count)
        outs[step][:count, :] = summed_ref[pl.ds(pl.multiple_of(peer * count, count), count), :]
        outs[step][count:, :] = stats_ref[pl.ds(pl.multiple_of(peer * half, half), half), :]


def far_kernel(mine_heads, rows, per_owner, scale, ask_ref, k_ref, v_ref, out_ref):
    lead = ask_ref.shape[0]
    prompt_count = k_ref.shape[0]
    stats = None
    for head in range(mine_heads):
        mine = ask_ref[:, head * rows : (head + 1) * rows, :]
        q = mine[:, :, :LANES].reshape(lead * rows, LANES)
        code = mine[:, :, LANES:].reshape(lead * rows, LANES).astype(jnp.float32)
        scores = jnp.full(code.shape, LOW, jnp.float32)
        masks = []
        for prompt in range(prompt_count):
            part = lax.dot_general(
                q, k_ref[prompt, head], (((1,), (1,)), ((), ())),
                preferred_element_type=jnp.float32,
            )
            for block in range(per_owner):
                mask = code == float(prompt * per_owner + block)
                masks.append(mask)
                scores = jnp.where(
                    mask, part[:, block * BLOCK : (block + 1) * BLOCK] * scale, scores
                )
        highest = jnp.max(scores, axis=1, keepdims=True)
        exponent = jnp.where(code >= 0.0, jnp.exp(scores - highest), 0.0)
        totals = jnp.sum(exponent, axis=1, keepdims=True)

        def values_of(index):
            prompt, block = divmod(index, per_owner)
            return v_ref[prompt, head, block * BLOCK : (block + 1) * BLOCK, :]

        summed = split_product(exponent, values_of, masks)
        out_ref[:, head * rows : (head + 1) * rows, :] = summed.reshape(lead, rows, LANES)
        tile = statistics(highest, totals, head, rows, lead)
        stats = tile if stats is None else stats + tile
    out_ref[:, mine_heads * rows :, :] = stats


def merge_kernel(row_count, mine_heads, per_kv, far_ref, *rest):
    near_refs, out_ref, rows_ref = rest[:-2], rest[-2], rest[-1]
    rows = per_kv * row_count
    half = rows // 2
    count = mine_heads * rows
    far_count = far_ref.shape[0]
    stats = [far_ref[index, count:, :] for index in range(far_count)]
    stats += [ref[count:, :] for ref in near_refs]
    peak = functools.reduce(jnp.maximum, stats)
    factors = [jnp.exp(tile - peak) for tile in stats]
    weight = None
    for tile, factor in zip(stats, factors):
        term = factor * pltpu.roll(tile, LANES // 2, 1)
        weight = term if weight is None else weight + term
    lane = lax.broadcasted_iota(jnp.int32, weight.shape, 1)
    weight = jnp.where(lane < 2 * mine_heads, weight, 1.0)
    factors = [factor / weight for factor in factors]
    for index in range(2 * mine_heads):
        at = slice(index * half, (index + 1) * half)
        total = None
        for part, factor in enumerate(factors):
            source = far_ref[part, at, :] if part < far_count else near_refs[part - far_count][at, :]
            term = factor[:, index : index + 1] * source
            total = term if total is None else total + term
        rows_ref[at, :] = total
    for head in range(mine_heads):
        for query in range(per_kv):
            tile = head * per_kv + query
            out_ref[:, tile * LANES : (tile + 1) * LANES] = rows_ref[
                pl.ds(head * rows + query, row_count, stride=per_kv), :
            ].astype(out_ref.dtype)


def partner(me, step, count):
    if count & (count - 1) == 0:
        return me ^ step
    return lax.rem(me + step, count)


def per_device(queries, request_of, selected, cache_keys, cache_values, recent_keys, recent_values):
    row_count = queries.shape[0]
    heads_kv = recent_keys.shape[1]
    near_tokens = recent_keys.shape[2]
    head_dim = recent_keys.shape[3]
    per_kv = queries.shape[1] // (heads_kv * head_dim)
    mine_heads = selected.shape[1]
    top_count = selected.shape[2]
    score_scale = head_dim ** (-0.5)
    owner_count = lax.axis_size("cache")
    group_count = lax.axis_size("group")
    prompt_count = cache_keys.shape[0]
    held = cache_keys.shape[2]
    per_owner = held // BLOCK
    rows = per_kv * row_count
    count = mine_heads * rows
    packed = count + rows // 2

    ask, query_rows = pl.pallas_call(
        functools.partial(ask_kernel, row_count, mine_heads, per_kv, top_count, per_owner),
        compiler_params=PARAMS,
        cost_estimate=pl.CostEstimate(flops=ASK_FLOPS, bytes_accessed=1 << 20, transcendentals=0),
        out_shape=[
            jax.ShapeDtypeStruct((owner_count, count, 2 * head_dim), queries.dtype),
            pltpu.VMEM((heads_kv * rows, head_dim), queries.dtype),
        ],
        in_specs=[IN_HBM] * 3,
        out_specs=[IN_VMEM] * 2,
        scratch_shapes=[
            pltpu.VMEM(queries.shape, queries.dtype),
            pltpu.SMEM(request_of.shape, request_of.dtype),
            pltpu.SMEM(selected.shape, selected.dtype),
            pltpu.VMEM((heads_kv * rows, head_dim), jnp.float32),
            pltpu.VMEM((owner_count, count, head_dim), jnp.float32),
            pltpu.SemaphoreType.DMA((3,)),
        ],
    )(stay(queries), stay(request_of), stay(selected))
    asked = lax.all_to_all(ask, "cache", split_axis=0, concat_axis=0, tiled=True)

    near = pl.pallas_call(
        functools.partial(near_kernel, row_count, mine_heads, per_kv, score_scale),
        compiler_params=PARAMS,
        out_shape=[pltpu.VMEM((packed, head_dim), jnp.float32)] * group_count,
        in_specs=[IN_VMEM, IN_VMEM, IN_HBM],
        out_specs=[IN_VMEM] * group_count,
        scratch_shapes=[
            pltpu.VMEM(recent_values.shape, recent_values.dtype),
            pltpu.VMEM((heads_kv * rows, near_tokens), jnp.float32),
            pltpu.VMEM((heads_kv * rows, head_dim), jnp.float32),
            pltpu.VMEM((group_count * rows // 2, head_dim), jnp.float32),
            pltpu.SemaphoreType.DMA((group_count,)),
        ],
    )(keep(query_rows), keep(recent_keys), stay(recent_values))
    near = [near[0]] + [
        lax.ppermute(
            near[step], "group", [(i, int(partner_of(i, step, group_count))) for i in range(group_count)]
        )
        for step in range(1, group_count)
    ]

    lead = min(owner_count, 8)
    if owner_count == lead:
        specs = dict(
            in_specs=[IN_VMEM] * 3,
            out_specs=IN_VMEM,
            out_shape=pltpu.VMEM((owner_count, packed, head_dim), jnp.float32),
        )
        asked = keep(asked)
    else:
        specs = dict(
            grid=(owner_count // lead,),
            in_specs=[pl.BlockSpec((lead, count, 2 * head_dim), lambda i: (i, 0, 0)), IN_VMEM, IN_VMEM],
            out_specs=pl.BlockSpec((lead, packed, head_dim), lambda i: (i, 0, 0)),
            out_shape=jax.ShapeDtypeStruct((owner_count, packed, head_dim), jnp.float32),
        )
    far = pl.pallas_call(
        functools.partial(far_kernel, mine_heads, rows, per_owner, score_scale), compiler_params=PARAMS, **specs
    )(asked, keep(cache_keys), keep(cache_values))

    far = lax.all_to_all(far, "cache", split_axis=0, concat_axis=0, tiled=True)

    return pl.pallas_call(
        functools.partial(merge_kernel, row_count, mine_heads, per_kv), compiler_params=PARAMS,
        out_shape=jax.ShapeDtypeStruct((row_count, count // row_count * head_dim), jnp.bfloat16),
        in_specs=[IN_VMEM] * (1 + group_count),
        out_specs=IN_VMEM,
        scratch_shapes=[pltpu.VMEM((count, head_dim), jnp.float32)],
    )(keep(far), *[keep(part) for part in near])


def partner_of(me, step, count):
    return me ^ step if count & (count - 1) == 0 else (me + step) % count


def solution(mesh):
    return jax.shard_map(
        per_device,
        mesh=mesh,
        in_specs=(
            P("cache", None),
            P("cache"),
            P("cache", "group", None),
            P(None, "group", "cache", None),
            P(None, "group", "cache", None),
            P("cache", None, "group", None),
            P("cache", None, "group", None),
        ),
        out_specs=P("cache", "group"),
        check_vma=False,
    )
```

```python
import functools

import jax
import jax.numpy as jnp
from jax import lax
from jax.experimental import pallas as pl
from jax.experimental.pallas import tpu as pltpu
from jax.sharding import PartitionSpec as P

BLOCK = 128
LANES = 128
LOW = -1e30

LONG = pl.CostEstimate(flops=10**9, bytes_accessed=1 << 20, transcendentals=0)
IN_VMEM = pl.BlockSpec(memory_space=pltpu.VMEM)
IN_HBM = pl.BlockSpec(memory_space=pl.ANY)


PARAMS = pltpu.CompilerParams(vmem_limit_bytes=16 * 1024 * 1024)


def stay(array):
    return pltpu.with_memory_space_constraint(array, pltpu.HBM)


def keep(array):
    return pltpu.with_memory_space_constraint(array, pltpu.VMEM)


def split_product(exponent, values_of, masks):
    rows = exponent.shape[0]
    high = exponent.astype(jnp.bfloat16).astype(jnp.float32)
    both = jnp.concatenate([high, exponent - high], axis=0)
    total = None
    for index, mask in enumerate(masks):
        part = jnp.where(jnp.concatenate([mask, mask], axis=0), both, 0.0).astype(jnp.bfloat16)
        term = jnp.dot(part, values_of(index), preferred_element_type=jnp.float32)
        total = term if total is None else total + term
    return total[:rows] + total[rows:]


def statistics(highest, totals, head, rows, lead):
    half_rows = rows // 2
    shape = (lead * rows, LANES)
    lane = lax.broadcasted_iota(jnp.int32, shape, 1)
    row = lax.broadcasted_iota(jnp.int32, shape, 0)
    place = 2 * head + (row % rows) // half_rows
    tile = jnp.where(lane == place, highest, 0.0) + jnp.where(
        lane == place + LANES // 2, totals, 0.0
    )
    tile = tile.reshape(lead, rows, LANES)
    return tile[:, :half_rows] + tile[:, half_rows:]


def ask_kernel(order, row_count, mine_heads, per_kv, top_count, per_owner, q_hbm, prompt_hbm, sel_hbm,
               out_ref, q_rows_ref, q_ref, prompt_ref, sel_ref, rows_ref, code_ref, sems):
    rows = row_count * per_kv
    pairs = ((q_hbm, q_ref), (prompt_hbm, prompt_ref), (sel_hbm, sel_ref))
    copies = [
        pltpu.make_async_copy(source, target, sems.at[index])
        for index, (source, target) in enumerate(pairs)
    ]
    for copy in copies:
        copy.start()
    code_ref[...] = jnp.full(code_ref.shape, -1.0, jnp.float32)
    for copy in copies:
        copy.wait()
    for tile in range(q_ref.shape[1] // LANES):
        head, query = divmod(tile, per_kv)
        rows_ref[pl.ds(head * rows + query, row_count, stride=per_kv), :] = q_ref[
            :, tile * LANES : (tile + 1) * LANES
        ].astype(jnp.float32)
    q_rows_ref[...] = rows_ref[...].astype(q_rows_ref.dtype)
    for head in range(mine_heads):
        for row in range(row_count):
            at = (head * row_count + row) * per_kv
            for top in range(top_count):
                block = sel_ref[row, head, top]
                owner = block // per_owner
                code = prompt_ref[row] * per_owner + block % per_owner
                code_ref[owner, at : at + per_kv, :] = jnp.full(
                    (per_kv, LANES), code, jnp.int32
                ).astype(jnp.float32)
    first = pl.multiple_of(lax.axis_index("group") * (mine_heads * rows), mine_heads * rows)
    mine = rows_ref[pl.ds(first, mine_heads * rows), :].astype(out_ref.dtype)
    for place, owner in enumerate(order):
        out_ref[place, :, :LANES] = mine
        out_ref[place, :, LANES:] = code_ref[owner].astype(out_ref.dtype)


def near_scores(row_count, per_kv, scale, q_ref, k_ref, out_ref):
    rows = per_kv * row_count
    slot = lax.broadcasted_iota(jnp.int32, (rows, 1), 0) // per_kv
    for head in range(out_ref.shape[0] // rows):
        at = slice(head * rows, (head + 1) * rows)
        q = q_ref[at, :]
        scores = None
        for row in range(row_count):
            part = lax.dot_general(
                q, k_ref[row, head], (((1,), (1,)), ((), ())), preferred_element_type=jnp.float32
            )
            scores = part if scores is None else jnp.where(slot == row, part, scores)
        out_ref[at, :] = scores * scale


def near_kernel(row_count, mine_heads, per_kv, scores_ref, v_ref, *rest):
    outs, (summed_ref, stats_ref) = rest[:-2], rest[-2:]
    heads = len(outs) * mine_heads
    me = lax.axis_index("group")
    rows = per_kv * row_count
    half = rows // 2
    count = mine_heads * rows
    slot = lax.broadcasted_iota(jnp.int32, (rows, 1), 0) // per_kv
    scores = scores_ref[...]
    highest = jnp.max(scores, axis=1, keepdims=True)
    exponent = jnp.exp(scores - highest)
    totals = jnp.sum(exponent, axis=1, keepdims=True)
    high = exponent.astype(jnp.bfloat16)
    low = (exponent - high.astype(jnp.float32)).astype(jnp.bfloat16)
    for head in range(heads):
        at = slice(head * rows, (head + 1) * rows)
        both = jnp.concatenate([high[at], low[at]], axis=0)
        summed = None
        for row in range(row_count):
            part = jnp.dot(both, v_ref[row, head], preferred_element_type=jnp.float32)
            part = part[:rows] + part[rows:]
            summed = part if summed is None else jnp.where(slot == row, part, summed)
        summed_ref[at, :] = summed
        tile = statistics(highest[at], totals[at], head % mine_heads, rows, 1)[0]
        at = slice(head // mine_heads * half, (head // mine_heads + 1) * half)
        stats_ref[at, :] = tile if head % mine_heads == 0 else stats_ref[at, :] + tile
    for step, out in enumerate(outs):
        peer = me ^ step
        out[:count, :] = summed_ref[pl.ds(pl.multiple_of(peer * count, count), count), :]
        out[count:, :] = stats_ref[pl.ds(pl.multiple_of(peer * half, half), half), :]


def far_kernel(
    row_count, mine_heads, per_kv, per_owner, scale, gridded,
    ask_ref, k_ref, v_ref, q_ref, near_k_ref, out_hbm, scores_ref, out_ref, sem
):
    rows = per_kv * row_count
    lead = ask_ref.shape[0]
    prompt_count = k_ref.shape[0]
    stats = None
    for head in range(mine_heads):
        mine = ask_ref[:, head * rows : (head + 1) * rows, :]
        q = mine[:, :, :LANES].reshape(lead * rows, LANES)
        code = mine[:, :, LANES:].reshape(lead * rows, LANES).astype(jnp.float32)
        scores = jnp.full(code.shape, LOW, jnp.float32)
        masks = []
        for prompt in range(prompt_count):
            part = lax.dot_general(
                q, k_ref[prompt, head], (((1,), (1,)), ((), ())),
                preferred_element_type=jnp.float32,
            )
            for block in range(per_owner):
                mask = code == float(prompt * per_owner + block)
                masks.append(mask)
                scores = jnp.where(
                    mask, part[:, block * BLOCK : (block + 1) * BLOCK] * scale, scores
                )
        highest = jnp.max(scores, axis=1, keepdims=True)
        exponent = jnp.where(code >= 0.0, jnp.exp(scores - highest), 0.0)
        totals = jnp.sum(exponent, axis=1, keepdims=True)

        def values_of(index):
            prompt, block = divmod(index, per_owner)
            return v_ref[prompt, head, block * BLOCK : (block + 1) * BLOCK, :]

        summed = split_product(exponent, values_of, masks)
        out_ref[:, head * rows : (head + 1) * rows, :] = summed.reshape(lead, rows, LANES)
        tile = statistics(highest, totals, head, rows, lead)
        stats = tile if stats is None else stats + tile
    out_ref[:, mine_heads * rows :, :] = stats
    near = functools.partial(near_scores, row_count, per_kv, scale, q_ref, near_k_ref, scores_ref)
    if gridded:
        at = pl.program_id(0)
        copy = pltpu.make_async_copy(out_ref, out_hbm.at[pl.ds(at * lead, lead)], sem)
        copy.start()
        pl.when(at == 0)(near)
    else:
        copy = pltpu.make_async_copy(out_ref, out_hbm, sem)
        copy.start()
        near()
    copy.wait()


def merge_kernel(row_count, mine_heads, per_kv, far_ref, *rest):
    near_refs, out_ref, rows_ref = rest[:-2], rest[-2], rest[-1]
    rows = per_kv * row_count
    half = rows // 2
    count = mine_heads * rows
    far_count = far_ref.shape[0]
    stats = [far_ref[index, count:, :] for index in range(far_count)]
    stats += [ref[count:, :] for ref in near_refs]
    peak = functools.reduce(jnp.maximum, stats)
    factors = [jnp.exp(tile - peak) for tile in stats]
    weight = None
    for tile, factor in zip(stats, factors):
        term = factor * pltpu.roll(tile, LANES // 2, 1)
        weight = term if weight is None else weight + term
    lane = lax.broadcasted_iota(jnp.int32, weight.shape, 1)
    weight = jnp.where(lane < 2 * mine_heads, weight, 1.0)
    factors = [factor / weight for factor in factors]
    for index in range(2 * mine_heads):
        at = slice(index * half, (index + 1) * half)
        total = None
        for part, factor in enumerate(factors):
            source = far_ref[part, at, :] if part < far_count else near_refs[part - far_count][at, :]
            term = factor[:, index : index + 1] * source
            total = term if total is None else total + term
        rows_ref[at, :] = total
    for head in range(mine_heads):
        for query in range(per_kv):
            tile = head * per_kv + query
            out_ref[:, tile * LANES : (tile + 1) * LANES] = rows_ref[
                pl.ds(head * rows + query, row_count, stride=per_kv), :
            ].astype(out_ref.dtype)


def middle_first(count):
    middle = list(range(count))[count // 2 : count // 2 + 2]
    return middle + [owner for owner in range(count) if owner not in middle]


def exchange(array, order):
    return lax.all_to_all(
        array, "cache", split_axis=0, concat_axis=0, tiled=True, axis_index_groups=[order]
    )


def per_device(queries, request_of, selected, cache_keys, cache_values, recent_keys, recent_values):
    row_count = queries.shape[0]
    heads_kv = recent_keys.shape[1]
    near_tokens = recent_keys.shape[2]
    head_dim = recent_keys.shape[3]
    per_kv = queries.shape[1] // (heads_kv * head_dim)
    mine_heads = selected.shape[1]
    top_count = selected.shape[2]
    score_scale = head_dim ** (-0.5)
    owner_count = lax.axis_size("cache")
    group_count = lax.axis_size("group")
    prompt_count = cache_keys.shape[0]
    held = cache_keys.shape[2]
    per_owner = held // BLOCK
    order = middle_first(owner_count)
    rows = per_kv * row_count
    count = mine_heads * rows
    packed = count + rows // 2

    ask, query_rows = pl.pallas_call(
        functools.partial(ask_kernel, order, row_count, mine_heads, per_kv, top_count, per_owner),
        compiler_params=PARAMS,
        cost_estimate=LONG,
        out_shape=[
            jax.ShapeDtypeStruct((owner_count, count, 2 * head_dim), queries.dtype),
            pltpu.VMEM((heads_kv * rows, head_dim), queries.dtype),
        ],
        in_specs=[IN_HBM] * 3,
        out_specs=[IN_VMEM] * 2,
        scratch_shapes=[
            pltpu.VMEM(queries.shape, queries.dtype),
            pltpu.SMEM(request_of.shape, request_of.dtype),
            pltpu.SMEM(selected.shape, selected.dtype),
            pltpu.VMEM((heads_kv * rows, head_dim), jnp.float32),
            pltpu.VMEM((owner_count, count, head_dim), jnp.float32),
            pltpu.SemaphoreType.DMA((3,)),
        ],
    )(stay(queries), stay(request_of), stay(selected))
    asked = exchange(ask, order)

    lead = min(owner_count, 8)
    gridded = owner_count > lead
    if gridded:
        specs = dict(
            grid=(owner_count // lead,),
            in_specs=[pl.BlockSpec((lead, count, 2 * head_dim), lambda i: (i, 0, 0))] + [IN_VMEM] * 4,
            out_specs=[IN_HBM, IN_VMEM],
        )
    else:
        asked = keep(asked)
        specs = dict(in_specs=[IN_VMEM] * 5, out_specs=[IN_HBM, IN_VMEM])
    far, scores = pl.pallas_call(
        functools.partial(far_kernel, row_count, mine_heads, per_kv, per_owner, score_scale, gridded),
        compiler_params=PARAMS,
        cost_estimate=LONG,
        out_shape=[
            jax.ShapeDtypeStruct((owner_count, packed, head_dim), jnp.float32),
            pltpu.VMEM((heads_kv * rows, near_tokens), jnp.float32),
        ],
        scratch_shapes=[
            pltpu.VMEM((lead, packed, head_dim), jnp.float32), pltpu.SemaphoreType.DMA(()),
        ],
        **specs,
    )(asked, keep(cache_keys), keep(cache_values), keep(query_rows), keep(recent_keys))
    far = exchange(far, order)

    near = pl.pallas_call(
        functools.partial(near_kernel, row_count, mine_heads, per_kv),
        compiler_params=PARAMS,
        out_shape=[pltpu.VMEM((packed, head_dim), jnp.float32)] * group_count,
        in_specs=[IN_VMEM] * 2,
        out_specs=[IN_VMEM] * group_count,
        scratch_shapes=[
            pltpu.VMEM((heads_kv * rows, head_dim), jnp.float32),
            pltpu.VMEM((group_count * rows // 2, head_dim), jnp.float32),
        ],
    )(keep(scores), keep(recent_values))
    near = [near[0]] + [
        lax.ppermute(near[step], "group", [(i, i ^ step) for i in range(group_count)])
        for step in range(1, group_count)
    ]

    return pl.pallas_call(
        functools.partial(merge_kernel, row_count, mine_heads, per_kv), compiler_params=PARAMS,
        out_shape=jax.ShapeDtypeStruct((row_count, count // row_count * head_dim), jnp.bfloat16),
        in_specs=[IN_VMEM] * (1 + group_count),
        out_specs=IN_VMEM,
        scratch_shapes=[pltpu.VMEM((count, head_dim), jnp.float32)],
    )(keep(far), *[keep(part) for part in near])


def solution(mesh):
    return jax.shard_map(
        per_device,
        mesh=mesh,
        in_specs=(
            P("cache", None),
            P("cache"),
            P("cache", "group", None),
            P(None, "group", "cache", None),
            P(None, "group", "cache", None),
            P("cache", None, "group", None),
            P("cache", None, "group", None),
        ),
        out_specs=P("cache", "group"),
        check_vma=False,
    )
```

```python
import functools

import jax
import jax.numpy as jnp
from jax import lax
from jax.experimental import pallas as pl
from jax.experimental.pallas import tpu as pltpu
from jax.sharding import PartitionSpec as P


BLOCK = 128
LANES = 128
LOW = -1e30

ASK_FLOPS = 10**9
IN_VMEM = pl.BlockSpec(memory_space=pltpu.VMEM)
IN_HBM = pl.BlockSpec(memory_space=pl.ANY)


PARAMS = pltpu.CompilerParams(vmem_limit_bytes=16 * 1024 * 1024)


def stay(array):
    return pltpu.with_memory_space_constraint(array, pltpu.HBM)


def keep(array):
    return pltpu.with_memory_space_constraint(array, pltpu.VMEM)


def split_product(exponent, values_of, masks):
    rows = exponent.shape[0]
    high = exponent.astype(jnp.bfloat16).astype(jnp.float32)
    both = jnp.concatenate([high, exponent - high], axis=0)
    total = None
    for index, mask in enumerate(masks):
        part = jnp.where(jnp.concatenate([mask, mask], axis=0), both, 0.0).astype(jnp.bfloat16)
        term = jnp.dot(part, values_of(index), preferred_element_type=jnp.float32)
        total = term if total is None else total + term
    return total[:rows] + total[rows:]


def statistics(highest, totals, head, rows, lead):
    half_rows = rows // 2
    shape = (lead * rows, LANES)
    lane = lax.broadcasted_iota(jnp.int32, shape, 1)
    row = lax.broadcasted_iota(jnp.int32, shape, 0)
    place = 2 * head + (row % rows) // half_rows
    tile = jnp.where(lane == place, highest, 0.0) + jnp.where(
        lane == place + LANES // 2, totals, 0.0
    )
    tile = tile.reshape(lead, rows, LANES)
    return tile[:, :half_rows] + tile[:, half_rows:]


def ask_kernel(order, row_count, mine_heads, per_kv, top_count, per_owner, q_hbm, prompt_hbm, sel_hbm,
               out_ref, q_rows_ref, q_ref, prompt_ref, sel_ref, rows_ref, code_ref, sems):
    rows = row_count * per_kv
    pairs = ((q_hbm, q_ref), (prompt_hbm, prompt_ref), (sel_hbm, sel_ref))
    copies = [
        pltpu.make_async_copy(source, target, sems.at[index])
        for index, (source, target) in enumerate(pairs)
    ]
    for copy in copies:
        copy.start()
    code_ref[...] = jnp.full(code_ref.shape, -1.0, jnp.float32)
    for copy in copies:
        copy.wait()
    for tile in range(q_ref.shape[1] // LANES):
        head, query = divmod(tile, per_kv)
        rows_ref[pl.ds(head * rows + query, row_count, stride=per_kv), :] = q_ref[
            :, tile * LANES : (tile + 1) * LANES
        ].astype(jnp.float32)
    q_rows_ref[...] = rows_ref[...].astype(q_rows_ref.dtype)
    for head in range(mine_heads):
        for row in range(row_count):
            at = (head * row_count + row) * per_kv
            for top in range(top_count):
                block = sel_ref[row, head, top]
                owner = block // per_owner
                code = prompt_ref[row] * per_owner + block % per_owner
                code_ref[owner, at : at + per_kv, :] = jnp.full(
                    (per_kv, LANES), code, jnp.int32
                ).astype(jnp.float32)
    first = pl.multiple_of(lax.axis_index("group") * (mine_heads * rows), mine_heads * rows)
    mine = rows_ref[pl.ds(first, mine_heads * rows), :].astype(out_ref.dtype)
    for place, owner in enumerate(order):
        out_ref[place, :, :LANES] = mine
        out_ref[place, :, LANES:] = code_ref[owner].astype(out_ref.dtype)


def near_kernel(row_count, mine_heads, per_kv, scale, q_ref, k_ref, v_hbm, *rest):
    outs, (v_ref, scores_ref, summed_ref, stats_ref, sems) = rest[:-5], rest[-5:]
    group_count = len(outs)
    heads = group_count * mine_heads
    me = lax.axis_index("group")
    rows = per_kv * row_count
    half = rows // 2
    copies = []
    for index in range(group_count):
        at = pl.ds(index * mine_heads, mine_heads)
        copies.append(pltpu.make_async_copy(v_hbm.at[:, at], v_ref.at[:, at], sems.at[index]))
        copies[index].start()
    slot = lax.broadcasted_iota(jnp.int32, (rows, 1), 0) // per_kv
    for head in range(heads):
        q = q_ref[head * rows : (head + 1) * rows, :]
        scores = None
        for row in range(row_count):
            part = lax.dot_general(
                q, k_ref[row, head], (((1,), (1,)), ((), ())), preferred_element_type=jnp.float32
            )
            scores = part if scores is None else jnp.where(slot == row, part, scores)
        scores_ref[head * rows : (head + 1) * rows, :] = scores
    scores = scores_ref[...] * scale
    highest = jnp.max(scores, axis=1, keepdims=True)
    exponent = jnp.exp(scores - highest)
    totals = jnp.sum(exponent, axis=1, keepdims=True)
    high = exponent.astype(jnp.bfloat16)
    rest_part = (exponent - high.astype(jnp.float32)).astype(jnp.bfloat16)
    for head in range(heads):
        if head % mine_heads == 0:
            copies[head // mine_heads].wait()
        at = slice(head * rows, (head + 1) * rows)
        both = jnp.concatenate([high[at], rest_part[at]], axis=0)
        summed = None
        for row in range(row_count):
            part = jnp.dot(both, v_ref[row, head], preferred_element_type=jnp.float32)
            part = part[:rows] + part[rows:]
            summed = part if summed is None else jnp.where(slot == row, part, summed)
        summed_ref[at, :] = summed
        tile = statistics(highest[at], totals[at], head % mine_heads, rows, 1)[0]
        at = slice(head // mine_heads * half, (head // mine_heads + 1) * half)
        stats_ref[at, :] = tile if head % mine_heads == 0 else stats_ref[at, :] + tile
    count = mine_heads * rows
    for step in range(group_count):
        peer = partner(me, step, group_count)
        outs[step][:count, :] = summed_ref[pl.ds(pl.multiple_of(peer * count, count), count), :]
        outs[step][count:, :] = stats_ref[pl.ds(pl.multiple_of(peer * half, half), half), :]


def far_kernel(mine_heads, rows, per_owner, scale, ask_ref, k_ref, v_ref, out_ref):
    lead = ask_ref.shape[0]
    prompt_count = k_ref.shape[0]
    stats = None
    for head in range(mine_heads):
        mine = ask_ref[:, head * rows : (head + 1) * rows, :]
        q = mine[:, :, :LANES].reshape(lead * rows, LANES)
        code = mine[:, :, LANES:].reshape(lead * rows, LANES).astype(jnp.float32)
        scores = jnp.full(code.shape, LOW, jnp.float32)
        masks = []
        for prompt in range(prompt_count):
            part = lax.dot_general(
                q, k_ref[prompt, head], (((1,), (1,)), ((), ())),
                preferred_element_type=jnp.float32,
            )
            for block in range(per_owner):
                mask = code == float(prompt * per_owner + block)
                masks.append(mask)
                scores = jnp.where(
                    mask, part[:, block * BLOCK : (block + 1) * BLOCK] * scale, scores
                )
        highest = jnp.max(scores, axis=1, keepdims=True)
        exponent = jnp.where(code >= 0.0, jnp.exp(scores - highest), 0.0)
        totals = jnp.sum(exponent, axis=1, keepdims=True)

        def values_of(index):
            prompt, block = divmod(index, per_owner)
            return v_ref[prompt, head, block * BLOCK : (block + 1) * BLOCK, :]

        summed = split_product(exponent, values_of, masks)
        out_ref[:, head * rows : (head + 1) * rows, :] = summed.reshape(lead, rows, LANES)
        tile = statistics(highest, totals, head, rows, lead)
        stats = tile if stats is None else stats + tile
    out_ref[:, mine_heads * rows :, :] = stats


def gather_kernel(mine_heads, parts_ref, out_ref):
    count = parts_ref.shape[0]
    half = parts_ref.shape[1] // (2 * mine_heads + 1)
    rows = 2 * mine_heads * half
    stats = [parts_ref[index, rows:, :] for index in range(count)]
    lane = lax.broadcasted_iota(jnp.int32, stats[0].shape, 1)
    peak = functools.reduce(jnp.maximum, stats)
    factors = [jnp.exp(tile - peak) for tile in stats]
    weights = [factor * pltpu.roll(tile, LANES // 2, 1) for tile, factor in zip(stats, factors)]
    weight = functools.reduce(jnp.add, weights)
    for index in range(2 * mine_heads):
        at = slice(index * half, (index + 1) * half)
        terms = [
            factor[:, index : index + 1] * parts_ref[part, at, :]
            for part, factor in enumerate(factors)
        ]
        out_ref[at, :] = functools.reduce(jnp.add, terms)
    out_ref[rows:, :] = jnp.where(lane < LANES // 2, peak, pltpu.roll(weight, LANES // 2, 1))


def merge_kernel(row_count, mine_heads, per_kv, *rest):
    near_refs, out_ref, rows_ref = rest[:-2], rest[-2], rest[-1]
    rows = per_kv * row_count
    half = rows // 2
    count = mine_heads * rows
    stats = [ref[count:, :] for ref in near_refs]
    peak = functools.reduce(jnp.maximum, stats)
    factors = [jnp.exp(tile - peak) for tile in stats]
    weight = None
    for tile, factor in zip(stats, factors):
        term = factor * pltpu.roll(tile, LANES // 2, 1)
        weight = term if weight is None else weight + term
    lane = lax.broadcasted_iota(jnp.int32, weight.shape, 1)
    weight = jnp.where(lane < 2 * mine_heads, weight, 1.0)
    factors = [factor / weight for factor in factors]
    for index in range(2 * mine_heads):
        at = slice(index * half, (index + 1) * half)
        total = None
        for ref, factor in zip(near_refs, factors):
            term = factor[:, index : index + 1] * ref[at, :]
            total = term if total is None else total + term
        rows_ref[at, :] = total
    for head in range(mine_heads):
        for query in range(per_kv):
            tile = head * per_kv + query
            out_ref[:, tile * LANES : (tile + 1) * LANES] = rows_ref[
                pl.ds(head * rows + query, row_count, stride=per_kv), :
            ].astype(out_ref.dtype)


def middle_first(count):
    middle = list(range(count))[count // 2 : count // 2 + 2]
    return middle + [owner for owner in range(count) if owner not in middle]


def exchange(array, order):
    return lax.all_to_all(
        array, "cache", split_axis=0, concat_axis=0, tiled=True, axis_index_groups=[order]
    )


def partner(me, step, count):
    if count & (count - 1) == 0:
        return me ^ step
    return lax.rem(me + step, count)


def work(queries, request_of, selected, cache_keys, cache_values, recent_keys, recent_values):
    row_count = queries.shape[0]
    heads_kv = recent_keys.shape[1]
    near_tokens = recent_keys.shape[2]
    head_dim = recent_keys.shape[3]
    per_kv = queries.shape[1] // (heads_kv * head_dim)
    mine_heads = selected.shape[1]
    top_count = selected.shape[2]
    score_scale = head_dim ** (-0.5)
    owner_count = lax.axis_size("cache")
    group_count = lax.axis_size("group")
    held = cache_keys.shape[2]
    per_owner = held // BLOCK
    order = middle_first(owner_count)
    rows = per_kv * row_count
    count = mine_heads * rows
    packed = count + rows // 2

    ask, query_rows = pl.pallas_call(
        functools.partial(ask_kernel, order, row_count, mine_heads, per_kv, top_count, per_owner),
        compiler_params=PARAMS,
        cost_estimate=pl.CostEstimate(flops=ASK_FLOPS, bytes_accessed=1 << 20, transcendentals=0),
        out_shape=[
            jax.ShapeDtypeStruct((owner_count, count, 2 * head_dim), queries.dtype),
            pltpu.VMEM((heads_kv * rows, head_dim), queries.dtype),
        ],
        in_specs=[IN_HBM] * 3,
        out_specs=[IN_VMEM] * 2,
        scratch_shapes=[
            pltpu.VMEM(queries.shape, queries.dtype),
            pltpu.SMEM(request_of.shape, request_of.dtype),
            pltpu.SMEM(selected.shape, selected.dtype),
            pltpu.VMEM((heads_kv * rows, head_dim), jnp.float32),
            pltpu.VMEM((owner_count, count, head_dim), jnp.float32),
            pltpu.SemaphoreType.DMA((3,)),
        ],
    )(stay(queries), stay(request_of), stay(selected))
    asked = exchange(ask, order)

    near = pl.pallas_call(
        functools.partial(near_kernel, row_count, mine_heads, per_kv, score_scale),
        compiler_params=PARAMS,
        out_shape=[pltpu.VMEM((packed, head_dim), jnp.float32)] * group_count,
        in_specs=[IN_VMEM, IN_VMEM, IN_HBM],
        out_specs=[IN_VMEM] * group_count,
        scratch_shapes=[
            pltpu.VMEM(recent_values.shape, recent_values.dtype),
            pltpu.VMEM((heads_kv * rows, near_tokens), jnp.float32),
            pltpu.VMEM((heads_kv * rows, head_dim), jnp.float32),
            pltpu.VMEM((group_count * rows // 2, head_dim), jnp.float32),
            pltpu.SemaphoreType.DMA((group_count,)),
        ],
    )(keep(query_rows), keep(recent_keys), stay(recent_values))
    own = near[0]
    asked, own = lax.optimization_barrier((asked, own))
    parts = [own]
    for step in range(1, group_count):
        parts.append(lax.ppermute(near[step], "group", [(i, i ^ step) for i in range(group_count)]))
    near = parts

    lead = min(owner_count, 8)
    if owner_count == lead:
        specs = dict(
            in_specs=[IN_VMEM] * 3,
            out_specs=IN_VMEM,
            out_shape=pltpu.VMEM((owner_count, packed, head_dim), jnp.float32),
        )
        asked = keep(asked)
    else:
        specs = dict(
            grid=(owner_count // lead,),
            in_specs=[pl.BlockSpec((lead, count, 2 * head_dim), lambda i: (i, 0, 0)), IN_VMEM, IN_VMEM],
            out_specs=pl.BlockSpec((lead, packed, head_dim), lambda i: (i, 0, 0)),
            out_shape=jax.ShapeDtypeStruct((owner_count, packed, head_dim), jnp.float32),
        )
    far = pl.pallas_call(
        functools.partial(far_kernel, mine_heads, rows, per_owner, score_scale), compiler_params=PARAMS, **specs
    )(asked, keep(cache_keys), keep(cache_values))

    far = exchange(far, order)
    far = pl.pallas_call(
        functools.partial(gather_kernel, mine_heads), compiler_params=PARAMS,
        out_shape=pltpu.VMEM((packed, head_dim), jnp.float32),
        in_specs=[IN_VMEM],
        out_specs=IN_VMEM,
    )(keep(far))

    return pl.pallas_call(
        functools.partial(merge_kernel, row_count, mine_heads, per_kv), compiler_params=PARAMS,
        out_shape=jax.ShapeDtypeStruct((row_count, count // row_count * head_dim), jnp.bfloat16),
        in_specs=[IN_VMEM] * (1 + group_count),
        out_specs=IN_VMEM,
        scratch_shapes=[pltpu.VMEM((count, head_dim), jnp.float32)],
    )(*[keep(part) for part in (far, *near)])


def solution(mesh):
    return jax.shard_map(
        work,
        mesh=mesh,
        in_specs=(
            P("cache", None),
            P("cache"),
            P("cache", "group", None),
            P(None, "group", "cache", None),
            P(None, "group", "cache", None),
            P("cache", None, "group", None),
            P("cache", None, "group", None),
        ),
        out_specs=P("cache", "group"),
        check_vma=False,
    )
```

```python
import functools

import jax
import jax.numpy as jnp
from jax import lax
from jax.experimental import pallas as pl
from jax.experimental.pallas import tpu as pltpu
from jax.sharding import PartitionSpec as P


BLOCK = 128
LANES = 128
LOW = -1e30

ASK_FLOPS = 10**9
IN_VMEM = pl.BlockSpec(memory_space=pltpu.VMEM)
IN_HBM = pl.BlockSpec(memory_space=pl.ANY)


PARAMS = pltpu.CompilerParams(vmem_limit_bytes=16 * 1024 * 1024)


def stay(array):
    return pltpu.with_memory_space_constraint(array, pltpu.HBM)


def keep(array):
    return pltpu.with_memory_space_constraint(array, pltpu.VMEM)


def split_product(exponent, values_of, masks):
    rows = exponent.shape[0]
    high = exponent.astype(jnp.bfloat16).astype(jnp.float32)
    both = jnp.concatenate([high, exponent - high], axis=0)
    total = None
    for index, mask in enumerate(masks):
        part = jnp.where(jnp.concatenate([mask, mask], axis=0), both, 0.0).astype(jnp.bfloat16)
        term = jnp.dot(part, values_of(index), preferred_element_type=jnp.float32)
        total = term if total is None else total + term
    return total[:rows] + total[rows:]


def statistics(highest, totals, head, rows, lead):
    half_rows = rows // 2
    shape = (lead * rows, LANES)
    lane = lax.broadcasted_iota(jnp.int32, shape, 1)
    row = lax.broadcasted_iota(jnp.int32, shape, 0)
    place = 2 * head + (row % rows) // half_rows
    tile = jnp.where(lane == place, highest, 0.0) + jnp.where(
        lane == place + LANES // 2, totals, 0.0
    )
    tile = tile.reshape(lead, rows, LANES)
    return tile[:, :half_rows] + tile[:, half_rows:]


def ask_kernel(order, row_count, mine_heads, per_kv, top_count, per_owner, q_hbm, prompt_hbm, sel_hbm,
               out_hbm, q_ref, prompt_ref, sel_ref, rows_ref, mine_ref, code_ref, codes_ref, sems):
    first = lax.axis_index("group") * (mine_heads * per_kv)
    pairs = ((q_hbm, q_ref), (prompt_hbm, prompt_ref), (sel_hbm, sel_ref))
    copies = [
        pltpu.make_async_copy(source, target, sems.at[index])
        for index, (source, target) in enumerate(pairs)
    ]
    for copy in copies:
        copy.start()
    code_ref[...] = jnp.full(code_ref.shape, -1.0, jnp.float32)
    copies[0].wait()
    for head in range(mine_heads):
        for query in range(per_kv):
            start = pl.multiple_of((first + head * per_kv + query) * LANES, LANES)
            at = head * row_count * per_kv + query
            rows_ref[pl.ds(at, row_count, stride=per_kv), :] = q_ref[
                :, pl.ds(start, LANES)
            ].astype(jnp.float32)
    mine_ref[...] = rows_ref[...].astype(mine_ref.dtype)
    sends = [
        pltpu.make_async_copy(mine_ref, out_hbm.at[place, :, :LANES], sems.at[3 + place])
        for place in range(len(order))
    ]
    for copy in sends:
        copy.start()
    for copy in copies[1:]:
        copy.wait()
    for head in range(mine_heads):
        for row in range(row_count):
            at = (head * row_count + row) * per_kv
            for top in range(top_count):
                block = sel_ref[row, head, top]
                owner = lax.div(block, per_owner)
                code = prompt_ref[row] * per_owner + lax.rem(block, per_owner)
                code_ref[owner, at : at + per_kv, :] = jnp.full(
                    (per_kv, LANES), code, jnp.int32
                ).astype(jnp.float32)
    for place, owner in enumerate(order):
        codes_ref[place] = code_ref[owner].astype(codes_ref.dtype)
    last = pltpu.make_async_copy(codes_ref, out_hbm.at[:, :, LANES:], sems.at[3 + len(order)])
    last.start()
    for copy in sends:
        copy.wait()
    last.wait()


def near_kernel(row_count, mine_heads, per_kv, scale, queries_ref, k_ref, v_hbm, *rest):
    outs, (v_ref, q_ref, scores_ref, summed_ref, stats_ref, sems) = rest[:-6], rest[-6:]
    group_count = len(outs)
    heads = group_count * mine_heads
    me = lax.axis_index("group")
    rows = per_kv * row_count
    half = rows // 2
    copies = []
    for index in range(group_count):
        at = pl.ds(index * mine_heads, mine_heads)
        copies.append(pltpu.make_async_copy(v_hbm.at[:, at], v_ref.at[:, at], sems.at[index]))
        copies[index].start()
    for tile in range(heads * per_kv):
        head, query = divmod(tile, per_kv)
        q_ref[pl.ds(head * rows + query, row_count, stride=per_kv), :] = queries_ref[
            :, tile * LANES : (tile + 1) * LANES
        ].astype(jnp.float32)
    slot = lax.broadcasted_iota(jnp.int32, (rows, 1), 0) // per_kv
    for head in range(heads):
        q = q_ref[head * rows : (head + 1) * rows, :].astype(queries_ref.dtype)
        scores = None
        for row in range(row_count):
            part = lax.dot_general(
                q, k_ref[row, head], (((1,), (1,)), ((), ())), preferred_element_type=jnp.float32
            )
            scores = part if scores is None else jnp.where(slot == row, part, scores)
        scores_ref[head * rows : (head + 1) * rows, :] = scores
    scores = scores_ref[...] * scale
    highest = jnp.max(scores, axis=1, keepdims=True)
    exponent = jnp.exp(scores - highest)
    totals = jnp.sum(exponent, axis=1, keepdims=True)
    high = exponent.astype(jnp.bfloat16)
    rest_part = (exponent - high.astype(jnp.float32)).astype(jnp.bfloat16)
    for head in range(heads):
        if head % mine_heads == 0:
            copies[head // mine_heads].wait()
        at = slice(head * rows, (head + 1) * rows)
        both = jnp.concatenate([high[at], rest_part[at]], axis=0)
        summed = None
        for row in range(row_count):
            part = jnp.dot(both, v_ref[row, head], preferred_element_type=jnp.float32)
            part = part[:rows] + part[rows:]
            summed = part if summed is None else jnp.where(slot == row, part, summed)
        summed_ref[at, :] = summed
        tile = statistics(highest[at], totals[at], head % mine_heads, rows, 1)[0]
        at = slice(head // mine_heads * half, (head // mine_heads + 1) * half)
        stats_ref[at, :] = tile if head % mine_heads == 0 else stats_ref[at, :] + tile
    count = mine_heads * rows
    for step in range(group_count):
        peer = partner(me, step, group_count)
        outs[step][:count, :] = summed_ref[pl.ds(pl.multiple_of(peer * count, count), count), :]
        outs[step][count:, :] = stats_ref[pl.ds(pl.multiple_of(peer * half, half), half), :]


def far_kernel(mine_heads, rows, per_owner, scale, ask_ref, k_ref, v_ref, out_ref):
    lead = ask_ref.shape[0]
    prompt_count = k_ref.shape[0]
    stats = None
    for head in range(mine_heads):
        mine = ask_ref[:, head * rows : (head + 1) * rows, :]
        q = mine[:, :, :LANES].reshape(lead * rows, LANES)
        code = mine[:, :, LANES:].reshape(lead * rows, LANES).astype(jnp.float32)
        scores = jnp.full(code.shape, LOW, jnp.float32)
        masks = []
        for prompt in range(prompt_count):
            part = lax.dot_general(
                q, k_ref[prompt, head], (((1,), (1,)), ((), ())),
                preferred_element_type=jnp.float32,
            )
            for block in range(per_owner):
                mask = code == float(prompt * per_owner + block)
                masks.append(mask)
                scores = jnp.where(
                    mask, part[:, block * BLOCK : (block + 1) * BLOCK] * scale, scores
                )
        highest = jnp.max(scores, axis=1, keepdims=True)
        exponent = jnp.where(code >= 0.0, jnp.exp(scores - highest), 0.0)
        totals = jnp.sum(exponent, axis=1, keepdims=True)

        def values_of(index):
            prompt, block = divmod(index, per_owner)
            return v_ref[prompt, head, block * BLOCK : (block + 1) * BLOCK, :]

        summed = split_product(exponent, values_of, masks)
        out_ref[:, head * rows : (head + 1) * rows, :] = summed.reshape(lead, rows, LANES)
        tile = statistics(highest, totals, head, rows, lead)
        stats = tile if stats is None else stats + tile
    out_ref[:, mine_heads * rows :, :] = stats


def gather_kernel(mine_heads, parts_ref, out_ref):
    count = parts_ref.shape[0]
    half = parts_ref.shape[1] // (2 * mine_heads + 1)
    rows = 2 * mine_heads * half
    stats = [parts_ref[index, rows:, :] for index in range(count)]
    lane = lax.broadcasted_iota(jnp.int32, stats[0].shape, 1)
    peak = functools.reduce(jnp.maximum, stats)
    factors = [jnp.exp(tile - peak) for tile in stats]
    weights = [factor * pltpu.roll(tile, LANES // 2, 1) for tile, factor in zip(stats, factors)]
    weight = functools.reduce(jnp.add, weights)
    for index in range(2 * mine_heads):
        at = slice(index * half, (index + 1) * half)
        terms = [
            factor[:, index : index + 1] * parts_ref[part, at, :]
            for part, factor in enumerate(factors)
        ]
        out_ref[at, :] = functools.reduce(jnp.add, terms)
    out_ref[rows:, :] = jnp.where(lane < LANES // 2, peak, pltpu.roll(weight, LANES // 2, 1))


def merge_kernel(row_count, mine_heads, per_kv, *rest):
    near_refs, out_ref, rows_ref = rest[:-2], rest[-2], rest[-1]
    rows = per_kv * row_count
    half = rows // 2
    count = mine_heads * rows
    stats = [ref[count:, :] for ref in near_refs]
    peak = functools.reduce(jnp.maximum, stats)
    factors = [jnp.exp(tile - peak) for tile in stats]
    weight = None
    for tile, factor in zip(stats, factors):
        term = factor * pltpu.roll(tile, LANES // 2, 1)
        weight = term if weight is None else weight + term
    lane = lax.broadcasted_iota(jnp.int32, weight.shape, 1)
    weight = jnp.where(lane < 2 * mine_heads, weight, 1.0)
    factors = [factor / weight for factor in factors]
    for index in range(2 * mine_heads):
        at = slice(index * half, (index + 1) * half)
        total = None
        for ref, factor in zip(near_refs, factors):
            term = factor[:, index : index + 1] * ref[at, :]
            total = term if total is None else total + term
        rows_ref[at, :] = total
    for head in range(mine_heads):
        for query in range(per_kv):
            tile = head * per_kv + query
            out_ref[:, tile * LANES : (tile + 1) * LANES] = rows_ref[
                pl.ds(head * rows + query, row_count, stride=per_kv), :
            ].astype(out_ref.dtype)


def middle_first(count):
    middle = count // 2
    order = [middle]
    for owner in [1, 0, middle + 1, middle - 1, middle - 2, *range(count)]:
        if 0 <= owner < count and owner not in order:
            order.append(owner)
    return order


def exchange(array, order):
    return lax.all_to_all(
        array, "cache", split_axis=0, concat_axis=0, tiled=True, axis_index_groups=[order]
    )


def partner(me, step, count):
    if count & (count - 1) == 0:
        return me ^ step
    return lax.rem(me + step, count)


def work(queries, request_of, selected, cache_keys, cache_values, recent_keys, recent_values):
    row_count = queries.shape[0]
    heads_kv = recent_keys.shape[1]
    near_tokens = recent_keys.shape[2]
    head_dim = recent_keys.shape[3]
    per_kv = queries.shape[1] // (heads_kv * head_dim)
    mine_heads = selected.shape[1]
    top_count = selected.shape[2]
    score_scale = head_dim ** (-0.5)
    owner_count = lax.axis_size("cache")
    group_count = lax.axis_size("group")
    held = cache_keys.shape[2]
    per_owner = held // BLOCK
    order = middle_first(owner_count)
    rows = per_kv * row_count
    count = mine_heads * rows
    packed = count + rows // 2

    ask = pl.pallas_call(
        functools.partial(ask_kernel, order, row_count, mine_heads, per_kv, top_count, per_owner),
        compiler_params=PARAMS,
        cost_estimate=pl.CostEstimate(flops=ASK_FLOPS, bytes_accessed=1 << 20, transcendentals=0),
        out_shape=jax.ShapeDtypeStruct((owner_count, count, 2 * head_dim), queries.dtype),
        in_specs=[IN_HBM] * 3,
        out_specs=IN_HBM,
        scratch_shapes=[
            pltpu.VMEM(queries.shape, queries.dtype),
            pltpu.SMEM(request_of.shape, request_of.dtype),
            pltpu.SMEM(selected.shape, selected.dtype),
            pltpu.VMEM((count, head_dim), jnp.float32),
            pltpu.VMEM((count, head_dim), queries.dtype),
            pltpu.VMEM((owner_count, count, head_dim), jnp.float32),
            pltpu.VMEM((owner_count, count, head_dim), queries.dtype),
            pltpu.SemaphoreType.DMA((4 + owner_count,)),
        ],
    )(stay(queries), stay(request_of), stay(selected))
    asked = exchange(ask, order)

    near = pl.pallas_call(
        functools.partial(near_kernel, row_count, mine_heads, per_kv, score_scale),
        compiler_params=PARAMS,
        out_shape=[pltpu.VMEM((packed, head_dim), jnp.float32)] * group_count,
        in_specs=[IN_VMEM, IN_VMEM, IN_HBM],
        out_specs=[IN_VMEM] * group_count,
        scratch_shapes=[
            pltpu.VMEM(recent_values.shape, recent_values.dtype),
            pltpu.VMEM((heads_kv * rows, head_dim), jnp.float32),
            pltpu.VMEM((heads_kv * rows, near_tokens), jnp.float32),
            pltpu.VMEM((heads_kv * rows, head_dim), jnp.float32),
            pltpu.VMEM((group_count * rows // 2, head_dim), jnp.float32),
            pltpu.SemaphoreType.DMA((group_count,)),
        ],
    )(keep(queries), keep(recent_keys), stay(recent_values))
    own = near[0]
    asked, own = lax.optimization_barrier((asked, own))
    parts = [own]
    for step in range(1, group_count):
        parts.append(lax.ppermute(near[step], "group", [(i, i ^ step) for i in range(group_count)]))
    near = parts

    lead = min(owner_count, 8)
    if owner_count == lead:
        specs = dict(
            in_specs=[IN_VMEM] * 3,
            out_specs=IN_VMEM,
            out_shape=pltpu.VMEM((owner_count, packed, head_dim), jnp.float32),
        )
        asked = keep(asked)
    else:
        specs = dict(
            grid=(owner_count // lead,),
            in_specs=[pl.BlockSpec((lead, count, 2 * head_dim), lambda i: (i, 0, 0)), IN_VMEM, IN_VMEM],
            out_specs=pl.BlockSpec((lead, packed, head_dim), lambda i: (i, 0, 0)),
            out_shape=jax.ShapeDtypeStruct((owner_count, packed, head_dim), jnp.float32),
        )
    far = pl.pallas_call(
        functools.partial(far_kernel, mine_heads, rows, per_owner, score_scale), compiler_params=PARAMS, **specs
    )(asked, keep(cache_keys), keep(cache_values))

    far = exchange(far, order)
    far = pl.pallas_call(
        functools.partial(gather_kernel, mine_heads), compiler_params=PARAMS,
        out_shape=pltpu.VMEM((packed, head_dim), jnp.float32),
        in_specs=[IN_VMEM],
        out_specs=IN_VMEM,
    )(keep(far))

    return pl.pallas_call(
        functools.partial(merge_kernel, row_count, mine_heads, per_kv), compiler_params=PARAMS,
        out_shape=jax.ShapeDtypeStruct((row_count, count // row_count * head_dim), jnp.bfloat16),
        in_specs=[IN_VMEM] * (1 + group_count),
        out_specs=IN_VMEM,
        scratch_shapes=[pltpu.VMEM((count, head_dim), jnp.float32)],
    )(*[keep(part) for part in (far, *near)])


def solution(mesh):
    return jax.shard_map(
        work,
        mesh=mesh,
        in_specs=(
            P("cache", None),
            P("cache"),
            P("cache", "group", None),
            P(None, "group", "cache", None),
            P(None, "group", "cache", None),
            P("cache", None, "group", None),
            P("cache", None, "group", None),
        ),
        out_specs=P("cache", "group"),
        check_vma=False,
    )
```
